32 devices in a mesh: wide: 4 (over y, x), narrow: 8 (over z, core).
Axes of the slice: x: 2, y: 2, z: 4, core: 2. Of those that a mesh axis runs over, the one named last changes fastest.
Arguments:
- mixture: bfloat16 [4, 64, 256, 256], P(None, ('wide', 'narrow')), may hold values from -30 to 30
- w_attn: bfloat16 [2, 4, 256, 256], replicated, may hold values from -2.625 to 2.625
- w_up: bfloat16 [2, 256, 1024], replicated, may hold values from -0.375 to 0.375
- w_down: bfloat16 [2, 1024, 256], replicated, may hold values from -0.1875 to 0.1875
- norm_gain: float32 [2, 2, 256], replicated, may hold values from 0.1 to 1.9
- norm_bias: float32 [2, 2, 256], replicated, may hold values from -3 to 3
- group_gain: float32 [2, 256], replicated, may hold values from 0.1 to 1.9
- group_bias: float32 [2, 256], replicated, may hold values from -3 to 3
Outputs:
- separated: bfloat16 [4, 64, 256, 256], P(None, ('wide', 'narrow'))
The draws below stay inside these ranges and needn't reach their ends.
All inputs are finite; a program needn't handle non-finite values.
Results may differ from the reference program's by a relative error of at most 0.0083.
Values may be sent and summed in bfloat16 or wider, within the bound.
A program may use at most 64 MiB of HBM per device.

```python
import math
import jax
import jax.numpy as jnp
from jax import lax

D = 256
HEADS = 8
FF = 1024
FRAMES = 256
MIX = 4
SEGMENTS = 64
N_WIDE = 4


def draw_mixture(key, part):
    keys = jax.random.split(jax.random.fold_in(key, 11), 5)
    seg_positions = jnp.arange(SEGMENTS, dtype=jnp.float32)
    frame_positions = jnp.arange(FRAMES, dtype=jnp.float32)
    period = SEGMENTS // N_WIDE
    residue_level = jnp.exp(jax.random.uniform(keys[0], (MIX, period), minval=math.log(0.05), maxval=0.0))
    loudness = jnp.tile(residue_level, (1, N_WIDE))
    loudness = loudness * jnp.exp(jax.random.uniform(keys[1], (MIX, SEGMENTS), minval=math.log(0.7), maxval=math.log(1.2)))
    loudness = loudness * jnp.exp(math.log(3.0) * (seg_positions / SEGMENTS - 0.5))
    frame_ramp = jnp.exp(math.log(3.0) * (frame_positions / FRAMES - 0.5))
    channel_scale = jnp.exp(jax.random.uniform(keys[2], (D,), minval=math.log(0.4), maxval=math.log(2.0)))
    colour = 0.6 * jnp.clip(jax.random.normal(keys[3], (MIX, SEGMENTS, D)), -4.0, 4.0)
    entries = jnp.clip(jax.random.normal(keys[4], (MIX, SEGMENTS, FRAMES, D)), -3.0, 3.0)
    seg_offset = 0.8 * seg_positions / SEGMENTS
    frame_offset = 0.8 * frame_positions / FRAMES
    values = entries * loudness[:, :, None, None] * frame_ramp[None, None, :, None] * channel_scale
    values = values + colour[:, :, None, :] + seg_offset[None, :, None, None] + frame_offset[None, None, :, None]
    return values.astype(jnp.bfloat16)


def draw_w_attn(key, part):
    first_key = jax.random.fold_in(jax.random.fold_in(key, 23), 0)
    base_draw = jnp.clip(jax.random.normal(first_key, (2, 4, D, D)), -4.0, 4.0) / math.sqrt(D)
    return base_draw.astype(jnp.bfloat16)


def gaussian(own_key, shape, width, bound, kind=jnp.bfloat16):
    values = width * jax.random.normal(own_key, shape, jnp.float32)
    return jnp.clip(values, min=-bound, max=bound).astype(kind)


def setup_inputs(seed: int = 0) -> dict:
    splits = jax.random.split(jax.random.key(seed), 9)
    return {
        "mixture": draw_mixture(jax.random.fold_in(splits[8], 71), 0),
        "w_attn": draw_w_attn(jax.random.fold_in(splits[8], 71), 0),
        "w_up": gaussian(splits[2], (2, D, FF), D ** -0.5, 0.375),
        "w_down": gaussian(splits[3], (2, FF, D), FF ** -0.5, 0.1875),
        "norm_gain": jnp.clip(1.0 + 0.18 * jax.random.normal(splits[4], (2, 2, D), jnp.float32), 0.1, 1.9),
        "norm_bias": gaussian(splits[5], (2, 2, D), 0.5, 3.0, jnp.float32),
        "group_gain": jnp.clip(1.0 + 0.18 * jax.random.normal(splits[6], (2, D), jnp.float32), 0.1, 1.9),
        "group_bias": gaussian(splits[7], (2, D), 0.5, 3.0, jnp.float32),
    }


EPSILON = 1e-05

def positions_table(seq_length, model_width):
    positions = jnp.arange(seq_length, dtype=jnp.float32)[:, None]
    freq_index = jnp.arange(model_width // 2, dtype=jnp.float32)[None, :]
    angles = positions * jnp.exp(freq_index * (-2.0 * math.log(10000.0) / model_width))
    return jnp.concatenate([jnp.sin(angles), jnp.cos(angles)], axis=1)

def layer_norm(values, gain_row, bias_row):
    mean_value = lax.optimization_barrier(jnp.mean(values, axis=-1, keepdims=True))
    centered = values - mean_value
    variance = lax.optimization_barrier(jnp.mean(centered * centered, axis=-1, keepdims=True))
    return centered * lax.rsqrt(variance + EPSILON) * gain_row + bias_row

def encoder_block(seq_block, pos_table, attn_weights, up_weight, down_weight, gains, biases):
    groups, seq_length, inner_count, model_width = seq_block.shape
    head_size = model_width // HEADS
    state_rows = seq_block.astype(jnp.float32) + pos_table[None, :, None, :]
    normed = layer_norm(state_rows, gains[0], biases[0]).astype(jnp.bfloat16).reshape(-1, model_width)

    def project(matrix):
        product = jnp.dot(normed, matrix, preferred_element_type=jnp.float32).astype(jnp.bfloat16)
        return product.reshape(groups, seq_length, inner_count, HEADS, head_size)
    queries = project(attn_weights[0])
    key_rows = project(attn_weights[1])
    value_rows = project(attn_weights[2])
    scores = jnp.einsum('alnhe,amnhe->anhlm', queries.astype(jnp.float32), key_rows.astype(jnp.float32))
    scores = scores * (1.0 / math.sqrt(head_size))
    shifted = jnp.exp(scores - lax.optimization_barrier(jnp.max(scores, axis=-1, keepdims=True)))
    weights = (shifted / lax.optimization_barrier(jnp.sum(shifted, axis=-1, keepdims=True))).astype(jnp.bfloat16)
    attended = jnp.einsum('anhlm,amnhe->alnhe', weights.astype(jnp.float32), value_rows.astype(jnp.float32))
    attended = attended.astype(jnp.bfloat16).reshape(-1, model_width)
    mixed = jnp.dot(attended, attn_weights[3], preferred_element_type=jnp.float32)
    state_after = state_rows + mixed.reshape(state_rows.shape)
    normed_two = layer_norm(state_after, gains[1], biases[1]).astype(jnp.bfloat16).reshape(-1, model_width)
    hidden = jax.nn.relu(jnp.dot(normed_two, up_weight, preferred_element_type=jnp.float32)).astype(jnp.bfloat16)
    output = jnp.dot(hidden, down_weight, preferred_element_type=jnp.float32)
    return state_after + output.reshape(state_after.shape)

def run_layer(seq_data, layer_index, w_attn, w_up, w_down, norm_gain, norm_bias, block_rows):
    seq_count, seq_length, inner_count, model_width = seq_data.shape
    per_block = math.gcd(seq_count, max(1, block_rows // (seq_length * inner_count)))
    pos_table = positions_table(seq_length, model_width)
    blocked = seq_data.reshape(seq_count // per_block, per_block, seq_length, inner_count, model_width)

    def apply_block(seq_block):
        return encoder_block(seq_block, pos_table, w_attn[layer_index], w_up[layer_index], w_down[layer_index], norm_gain[layer_index], norm_bias[layer_index])
    return lax.map(apply_block, blocked).reshape(seq_count, seq_length, inner_count, model_width)

def group_norm(values, gain_row, bias_row):
    cell_count = values.shape[1] * values.shape[2] * values.shape[3]
    mean_value = lax.optimization_barrier(jnp.sum(values, axis=(1, 2, 3), keepdims=True)) / cell_count
    centered = values - mean_value
    variance = lax.optimization_barrier(jnp.sum(centered * centered, axis=(1, 2, 3), keepdims=True)) / cell_count
    return centered * lax.rsqrt(variance + EPSILON) * gain_row + bias_row

def reference(mixture, w_attn, w_up, w_down, norm_gain, norm_bias, group_gain, group_bias):
    mix_count, seg_count, frame_count, model_width = mixture.shape
    intra_out = run_layer(mixture.reshape(mix_count * seg_count, frame_count, 1, model_width), 0, w_attn, w_up, w_down, norm_gain, norm_bias, 8192).reshape(mixture.shape)
    carried = (group_norm(intra_out, group_gain[0], group_bias[0]) + mixture.astype(jnp.float32)).astype(jnp.bfloat16)
    turned = jnp.transpose(carried, (0, 2, 1, 3)).reshape(mix_count * frame_count, seg_count, 1, model_width)
    inter_out = run_layer(turned, 1, w_attn, w_up, w_down, norm_gain, norm_bias, 8192).astype(jnp.bfloat16)
    inter_out = jnp.transpose(inter_out.reshape(mix_count, frame_count, seg_count, model_width), (0, 2, 1, 3))
    separated = group_norm(inter_out.astype(jnp.float32), group_gain[1], group_bias[1]) + carried.astype(jnp.float32)
    return separated.astype(jnp.bfloat16)
```

```python
import functools
import math

import jax
import jax.numpy as jnp
from jax import lax
from jax.experimental import pallas as pl
from jax.experimental.pallas import tpu as pltpu
from jax.sharding import PartitionSpec as P

HEADS = 8
MESH = pl.DeviceIdType.MESH


EPSILON = 1e-05


def positions_table(seq_length, model_width):
    positions = jnp.arange(seq_length, dtype=jnp.float32)[:, None]
    freq_index = jnp.arange(model_width // 2, dtype=jnp.float32)[None, :]
    angles = positions * jnp.exp(freq_index * (-2.0 * math.log(10000.0) / model_width))
    return jnp.concatenate([jnp.sin(angles), jnp.cos(angles)], axis=1)


def layer_norm(values, gain_row, bias_row):
    mean_value = jnp.mean(values, axis=-1, keepdims=True)
    centered = values - mean_value
    variance = jnp.mean(centered * centered, axis=-1, keepdims=True)
    return centered * lax.rsqrt(variance + EPSILON) * gain_row + bias_row


def encoder_block(seq_block, pos_table, attn_weights, up_weight, down_weight, gains, biases):
    groups, seq_length, inner_count, model_width = seq_block.shape
    head_size = model_width // HEADS
    state_rows = seq_block.astype(jnp.float32) + pos_table[None, :, None, :]
    normed = (
        layer_norm(state_rows, gains[0], biases[0]).astype(jnp.bfloat16).reshape(-1, model_width)
    )

    def project(matrix):
        product = jnp.dot(normed, matrix, preferred_element_type=jnp.float32).astype(jnp.bfloat16)
        return product.reshape(groups, seq_length, inner_count, HEADS, head_size)

    queries = project(attn_weights[0])
    key_rows = project(attn_weights[1])
    value_rows = project(attn_weights[2])
    scores = jnp.einsum("alnhe,amnhe->anhlm", queries, key_rows, preferred_element_type=jnp.float32)
    scores = scores * (1.0 / math.sqrt(head_size))
    shifted = jnp.exp(scores - jnp.max(scores, axis=-1, keepdims=True))
    weights = (shifted / jnp.sum(shifted, axis=-1, keepdims=True)).astype(jnp.bfloat16)
    attended = jnp.einsum(
        "anhlm,amnhe->alnhe", weights, value_rows, preferred_element_type=jnp.float32
    )
    attended = attended.astype(jnp.bfloat16).reshape(-1, model_width)
    mixed = jnp.dot(attended, attn_weights[3], preferred_element_type=jnp.float32)
    state_after = state_rows + mixed.reshape(state_rows.shape)
    normed_two = (
        layer_norm(state_after, gains[1], biases[1]).astype(jnp.bfloat16).reshape(-1, model_width)
    )
    hidden = jax.nn.relu(jnp.dot(normed_two, up_weight, preferred_element_type=jnp.float32)).astype(
        jnp.bfloat16
    )
    output = jnp.dot(hidden, down_weight, preferred_element_type=jnp.float32)
    return state_after + output.reshape(state_after.shape)


def run_layer(seq_data, layer_index, w_attn, w_up, w_down, norm_gain, norm_bias, block_rows):
    seq_count, seq_length, inner_count, model_width = seq_data.shape
    per_block = math.gcd(seq_count, max(1, block_rows // (seq_length * inner_count)))
    pos_table = positions_table(seq_length, model_width)
    blocked = seq_data.reshape(
        seq_count // per_block, per_block, seq_length, inner_count, model_width
    )

    def apply_block(seq_block):
        return encoder_block(
            seq_block,
            pos_table,
            w_attn[layer_index],
            w_up[layer_index],
            w_down[layer_index],
            norm_gain[layer_index],
            norm_bias[layer_index],
        )

    return lax.map(apply_block, blocked).reshape(seq_count, seq_length, inner_count, model_width)


def group_norm(values, gain_row, bias_row):
    cell_count = (
        values.shape[1] * lax.axis_size(("wide", "narrow")) * values.shape[2] * values.shape[3]
    )
    totals, squares = lax.psum(
        (jnp.sum(values, axis=(1, 2, 3)), jnp.sum(values * values, axis=(1, 2, 3))),
        ("wide", "narrow"),
    )
    mean_flat = totals / cell_count
    variance = squares / cell_count - mean_flat * mean_flat
    centered = values - mean_flat[:, None, None, None]
    return centered * lax.rsqrt(variance[:, None, None, None] + EPSILON) * gain_row + bias_row


def on_device(mixture, w_attn, w_up, w_down, norm_gain, norm_bias, group_gain, group_bias):
    mix_count, segs_here, frame_count, model_width = mixture.shape
    intra_out = run_layer(
        mixture.reshape(mix_count * segs_here, frame_count, 1, model_width),
        0,
        w_attn,
        w_up,
        w_down,
        norm_gain,
        norm_bias,
        512,
    ).reshape(mixture.shape)
    carried = (
        group_norm(intra_out, group_gain[0], group_bias[0]) + mixture.astype(jnp.float32)
    ).astype(jnp.bfloat16)
    result = run_layer(
        lax.all_to_all(carried, ("wide", "narrow"), split_axis=2, concat_axis=1, tiled=True),
        1,
        w_attn,
        w_up,
        w_down,
        norm_gain,
        norm_bias,
        512,
    ).astype(jnp.bfloat16)
    inter_out = lax.all_to_all(result, ("wide", "narrow"), split_axis=1, concat_axis=2, tiled=True)
    separated = group_norm(
        inter_out.astype(jnp.float32), group_gain[1], group_bias[1]
    ) + carried.astype(jnp.float32)
    return separated.astype(jnp.bfloat16)


def pick_sizes(mixture, device_count):
    _, segs_here, frame_count, model_width = mixture.shape
    seq_length = segs_here * device_count
    frames_here = frame_count // device_count
    group_rows = min(frame_count, seq_length * frames_here)
    fits = (
        frames_here == 8
        and frame_count % 128 == 0
        and 128 % seq_length == 0
        and group_rows % 128 == 0
        and (seq_length * frames_here) % group_rows == 0
        and model_width % 128 == 0
        and 128 % (model_width // HEADS) == 0
    )
    return fits, seq_length, frames_here, group_rows


def dot(left, right, left_dim=1, right_dim=0):
    return lax.dot_general(
        left, right, (((left_dim,), (right_dim,)), ((), ())), preferred_element_type=jnp.float32
    )


def group_layer(state_rows, seq_length, attn, up_weight, down_weight, gains, biases):
    rows, model_width = state_rows.shape
    head_size = model_width // HEADS
    heads_in_tile = 128 // head_size
    scale = math.log2(math.e) / math.sqrt(head_size)
    normed = layer_norm(state_rows, gains[0:1], biases[0:1]).astype(jnp.bfloat16)
    queries = dot(attn(0), normed, 1, 1).astype(jnp.bfloat16)
    key_rows = dot(normed, attn(1)).astype(jnp.bfloat16)
    value_cols = dot(attn(2), normed, 1, 1).astype(jnp.bfloat16)
    zero_rows = jnp.zeros((head_size, rows), jnp.bfloat16)
    packed = seq_length < rows
    if packed:
        lane_seq = lax.broadcasted_iota(jnp.int32, (seq_length, 128), 1) // seq_length
        seqs_in_tile = 128 // seq_length
    parts = []
    for head in range(HEADS):
        tile, place = divmod(head, heads_in_tile)
        own = queries[head * head_size : (head + 1) * head_size]
        spread = jnp.concatenate(
            [own if i == place else zero_rows for i in range(heads_in_tile)], axis=0
        )
        scores = dot(key_rows[:, tile * 128 : (tile + 1) * 128], spread)
        if packed:
            columns = []
            for lane_tile in range(rows // 128):
                block = None
                for i in range(seqs_in_tile):
                    first = (lane_tile * seqs_in_tile + i) * seq_length
                    piece = scores[
                        first : first + seq_length, lane_tile * 128 : (lane_tile + 1) * 128
                    ]
                    block = piece if block is None else jnp.where(lane_seq == i, piece, block)
                columns.append(block)
            scores = jnp.concatenate(columns, axis=1)
        shifted = jnp.exp2((scores - jnp.max(scores, axis=0, keepdims=True)) * scale)
        inverse = 1.0 / jnp.sum(shifted, axis=0, keepdims=True)
        if packed:
            row_blocks = []
            for seq in range(rows // seq_length):
                lane_tile, i = divmod(seq, seqs_in_tile)
                kept = jnp.where(
                    lane_seq == i, shifted[:, lane_tile * 128 : (lane_tile + 1) * 128], 0.0
                )
                none = jnp.zeros_like(kept)
                row_blocks.append(
                    jnp.concatenate(
                        [kept if t == lane_tile else none for t in range(rows // 128)], axis=1
                    )
                )
            shifted = jnp.concatenate(row_blocks, axis=0)
        attended = dot(
            value_cols[head * head_size : (head + 1) * head_size], shifted.astype(jnp.bfloat16)
        )
        parts.append((attended * inverse).astype(jnp.bfloat16))
    mixed = dot(jnp.concatenate(parts, axis=0), attn(3), 0, 0)
    state_after = state_rows + mixed
    normed_two = layer_norm(state_after, gains[1:2], biases[1:2]).astype(jnp.bfloat16)
    hidden = jnp.maximum(dot(normed_two, up_weight), 0.0).astype(jnp.bfloat16)
    return state_after + dot(hidden, down_weight)


def lane_sums(values):
    column = jnp.sum(values, axis=0, keepdims=True)
    total = column[:, 0:128]
    for tile in range(1, values.shape[1] // 128):
        total = total + column[:, tile * 128 : (tile + 1) * 128]
    return total


def fused_kernel(
    axis_names,
    axis_sizes,
    seq_length,
    frames_here,
    group_rows,
    x_ref,
    attn_ref,
    up_ref,
    down_ref,
    ngain_ref,
    nbias_ref,
    ggain_ref,
    gbias_ref,
    pos0_ref,
    pos1_ref,
    out_ref,
    y_scr,
    carried_scr,
    recv_scr,
    inter_scr,
    back_scr,
    rows_scr,
    stat_scr,
    send_sem,
    recv_sem,
):
    mixes, segs_here, frame_count, model_width = x_ref.shape
    n = axis_sizes[0] * axis_sizes[1]
    me = lax.axis_index(axis_names[0]) * axis_sizes[1] + lax.axis_index(axis_names[1])
    cells = float(n * segs_here * frame_count * model_width)
    lane_tiles = model_width // 128

    def device_of(index):
        return (index // axis_sizes[1], lax.rem(index, axis_sizes[1]))

    barrier = pltpu.get_barrier_semaphore()

    def greet(k, carry):
        pl.semaphore_signal(
            barrier, inc=1, device_id=device_of(lax.rem(me + k, n)), device_id_type=MESH
        )
        return carry

    lax.fori_loop(1, n, greet, 0)

    def send_all(kind, b, source, target):
        def send(k, carry):
            peer = lax.rem(me + k, n)
            pltpu.make_async_remote_copy(
                src_ref=source(peer),
                dst_ref=target(),
                send_sem=send_sem.at[kind, b],
                recv_sem=recv_sem.at[kind, b],
                device_id=device_of(peer),
                device_id_type=MESH,
            ).start()
            return carry

        lax.fori_loop(1, n, send, 0)

    def arrived(ref, sem):
        pltpu.make_async_copy(ref, ref, sem).wait()

    def stat_block(which, b):
        return stat_scr.at[which, b, pl.ds(0, n - 1)]

    def share_stats(which, b, sums, squares):
        stat_scr[which, b, me, 0:1, :] = sums
        stat_scr[which, b, me, 1:2, :] = squares
        send_all(
            which,
            b,
            lambda peer: stat_scr.at[which, b, me],
            lambda: stat_scr.at[which, b, me],
        )

    def affine(which, b):
        arrived(stat_block(which, b), recv_sem.at[which, b])
        total = jnp.sum(stat_scr[which, b], axis=0)
        flat = jnp.sum(total, axis=1, keepdims=True) / cells
        mean = flat[0:1]
        variance = flat[1:2] - mean * mean
        gain = lax.rsqrt(variance + EPSILON) * ggain_ref[which : which + 1]
        return gain, gbias_ref[which : which + 1] - mean * gain

    def weights(layer):
        return (
            lambda i: attn_ref[layer, i],
            up_ref[layer],
            down_ref[layer],
            ngain_ref[layer],
            nbias_ref[layer],
        )

    def intra(b):
        def one(c, sums):
            state = x_ref[b, c].astype(jnp.float32) + pos0_ref[...]
            y = group_layer(state, frame_count, *weights(0))
            y_scr[b, c] = y
            return sums[0] + lane_sums(y), sums[1] + lane_sums(y * y)

        zero = jnp.zeros((1, 128), jnp.float32)
        return lax.fori_loop(0, segs_here, one, (zero, zero))

    def carry_out(b):
        gain, bias = affine(0, b)

        def one(c, carry):
            full = y_scr[b, c] * gain + bias + x_ref[b, c].astype(jnp.float32)
            carried_scr[b, c] = full.reshape(n, frames_here, model_width).astype(jnp.bfloat16)
            return carry

        lax.fori_loop(0, segs_here, one, 0)
        recv_scr[b, pl.ds(me * segs_here, segs_here)] = carried_scr[b, :, me]
        send_all(
            2,
            b,
            lambda peer: carried_scr.at[b, :, peer],
            lambda: recv_scr.at[b, pl.ds(me * segs_here, segs_here)],
        )

    def first_half(step, carry):
        @pl.when(step < mixes)
        def _():
            sums, squares = intra(step)

            @pl.when(step == 0)
            def _():
                pl.semaphore_wait(barrier, n - 1)

            share_stats(0, step, sums, squares)

        @pl.when(step >= 1)
        def _():
            carry_out(step - 1)

        return carry

    lax.fori_loop(0, mixes + 1, first_half, 0)

    seqs = group_rows // seq_length

    def inter(b, carry):
        arrived(recv_scr.at[b, pl.ds(0, (n - 1) * segs_here)], recv_sem.at[2, b])
        wide_rows = recv_scr[b].astype(jnp.float32).reshape(seq_length * frames_here, model_width)
        for t in range(lane_tiles):
            rows_scr[t] = wide_rows[:, t * 128 : (t + 1) * 128]

        def one(g, sums):
            blocks = []
            for i in range(seqs):
                picked = [
                    rows_scr[t, pl.ds(g * seqs + i, seq_length, stride=frames_here), :]
                    for t in range(lane_tiles)
                ]
                blocks.append(jnp.concatenate(picked, axis=1) + pos1_ref[...])
            y = group_layer(jnp.concatenate(blocks, axis=0), seq_length, *weights(1))
            y = y.astype(jnp.bfloat16).astype(jnp.float32)
            for i in range(seqs):
                for t in range(lane_tiles):
                    rows_scr[t, pl.ds(g * seqs + i, seq_length, stride=frames_here), :] = y[
                        i * seq_length : (i + 1) * seq_length, t * 128 : (t + 1) * 128
                    ]
            return sums[0] + lane_sums(y), sums[1] + lane_sums(y * y)

        zero = jnp.zeros((1, 128), jnp.float32)
        sums, squares = lax.fori_loop(0, frames_here // seqs, one, (zero, zero))
        for t in range(lane_tiles):
            inter_scr[b, :, :, t * 128 : (t + 1) * 128] = (
                rows_scr[t].reshape(seq_length, frames_here, 128).astype(jnp.bfloat16)
            )
        back_scr[b, :, me] = inter_scr[b, pl.ds(me * segs_here, segs_here)]
        share_stats(1, b, sums, squares)
        send_all(
            3,
            b,
            lambda peer: inter_scr.at[b, pl.ds(peer * segs_here, segs_here)],
            lambda: back_scr.at[b, :, me],
        )
        return carry

    lax.fori_loop(0, mixes, inter, 0)

    def finish(b, carry):
        gain, bias = affine(1, b)
        arrived(back_scr.at[b, :, pl.ds(0, n - 1)], recv_sem.at[3, b])

        def one(c, inner):
            full = back_scr[b, c].astype(jnp.float32) * gain + bias
            full = full + carried_scr[b, c].astype(jnp.float32)
            out_ref[b, c] = full.reshape(frame_count, model_width).astype(jnp.bfloat16)
            return inner

        lax.fori_loop(0, segs_here, one, 0)
        arrived(stat_block(0, b), send_sem.at[0, b])
        arrived(stat_block(1, b), send_sem.at[1, b])
        arrived(carried_scr.at[b, :, pl.ds(0, n - 1)], send_sem.at[2, b])
        arrived(inter_scr.at[b, pl.ds(0, (n - 1) * segs_here)], send_sem.at[3, b])
        return carry

    lax.fori_loop(0, mixes, finish, 0)


def fused(mesh, mixture, w_attn, w_up, w_down, norm_gain, norm_bias, group_gain, group_bias):
    axis_names = ("wide", "narrow")
    axis_sizes = tuple(mesh.shape[name] for name in axis_names)
    n = axis_sizes[0] * axis_sizes[1]
    mixes, segs_here, frame_count, model_width = mixture.shape
    _, seq_length, frames_here, group_rows = pick_sizes(mixture, n)
    turned = jnp.swapaxes(w_attn, 2, 3)
    attn = jnp.stack([turned[:, 0], w_attn[:, 1], turned[:, 2], w_attn[:, 3]], axis=1)
    split = (mixes, segs_here, n, frames_here, model_width)
    joined = (mixes, seq_length, frames_here, model_width)
    return pl.pallas_call(
        functools.partial(
            fused_kernel, axis_names, axis_sizes, seq_length, frames_here, group_rows
        ),
        out_shape=jax.ShapeDtypeStruct(mixture.shape, jnp.bfloat16),
        in_specs=[pl.BlockSpec(memory_space=pltpu.VMEM)] * 10,
        out_specs=pl.BlockSpec(memory_space=pltpu.VMEM),
        scratch_shapes=[
            pltpu.VMEM(mixture.shape, jnp.float32),
            pltpu.VMEM(split, jnp.bfloat16),
            pltpu.VMEM(joined, jnp.bfloat16),
            pltpu.VMEM(joined, jnp.bfloat16),
            pltpu.VMEM(split, jnp.bfloat16),
            pltpu.VMEM((model_width // 128, seq_length * frames_here, 128), jnp.float32),
            pltpu.VMEM((2, mixes, n, 2, 128), jnp.float32),
            pltpu.SemaphoreType.DMA((4, mixes)),
            pltpu.SemaphoreType.DMA((4, mixes)),
        ],
        compiler_params=pltpu.CompilerParams(
            collective_id=0, has_side_effects=True, vmem_limit_bytes=60 * 1024 * 1024
        ),
    )(
        mixture,
        attn,
        w_up,
        w_down,
        norm_gain,
        norm_bias,
        group_gain,
        group_bias,
        positions_table(frame_count, model_width),
        positions_table(seq_length, model_width),
    )


def solution(mesh):
    in_specs = (P(None, ("wide", "narrow"), None, None), P(), P(), P(), P(), P(), P(), P())
    out_specs = P(None, ("wide", "narrow"), None, None)

    def step(mixture, *parameters):
        device_count = mesh.shape["wide"] * mesh.shape["narrow"]
        if pick_sizes(mixture, device_count)[0]:
            return fused(mesh, mixture, *parameters)
        return on_device(mixture, *parameters)

    return jax.shard_map(step, mesh=mesh, in_specs=in_specs, out_specs=out_specs, check_vma=False)
```

```python
import functools
import math

import jax
import jax.numpy as jnp
import numpy as np
from jax import lax
from jax.experimental import pallas as pl
from jax.experimental.pallas import tpu as pltpu
from jax.sharding import PartitionSpec as P

HEADS = 8
MESH = pl.DeviceIdType.MESH


EPSILON = 1e-05


def positions_table(seq_length, model_width):
    positions = jnp.arange(seq_length, dtype=jnp.float32)[:, None]
    freq_index = jnp.arange(model_width // 2, dtype=jnp.float32)[None, :]
    angles = positions * jnp.exp(freq_index * (-2.0 * math.log(10000.0) / model_width))
    return jnp.concatenate([jnp.sin(angles), jnp.cos(angles)], axis=1)


def layer_norm(values, gain_row, bias_row):
    mean_value = jnp.mean(values, axis=-1, keepdims=True)
    centered = values - mean_value
    variance = jnp.mean(centered * centered, axis=-1, keepdims=True)
    return centered * lax.rsqrt(variance + EPSILON) * gain_row + bias_row


def encoder_block(seq_block, pos_table, attn_weights, up_weight, down_weight, gains, biases):
    groups, seq_length, inner_count, model_width = seq_block.shape
    head_size = model_width // HEADS
    state_rows = seq_block.astype(jnp.float32) + pos_table[None, :, None, :]
    normed = (
        layer_norm(state_rows, gains[0], biases[0]).astype(jnp.bfloat16).reshape(-1, model_width)
    )

    def project(matrix):
        product = jnp.dot(normed, matrix, preferred_element_type=jnp.float32).astype(jnp.bfloat16)
        return product.reshape(groups, seq_length, inner_count, HEADS, head_size)

    queries = project(attn_weights[0])
    key_rows = project(attn_weights[1])
    value_rows = project(attn_weights[2])
    scores = jnp.einsum("alnhe,amnhe->anhlm", queries, key_rows, preferred_element_type=jnp.float32)
    scores = scores * (1.0 / math.sqrt(head_size))
    shifted = jnp.exp(scores - jnp.max(scores, axis=-1, keepdims=True))
    weights = (shifted / jnp.sum(shifted, axis=-1, keepdims=True)).astype(jnp.bfloat16)
    attended = jnp.einsum(
        "anhlm,amnhe->alnhe", weights, value_rows, preferred_element_type=jnp.float32
    )
    attended = attended.astype(jnp.bfloat16).reshape(-1, model_width)
    mixed = jnp.dot(attended, attn_weights[3], preferred_element_type=jnp.float32)
    state_after = state_rows + mixed.reshape(state_rows.shape)
    normed_two = (
        layer_norm(state_after, gains[1], biases[1]).astype(jnp.bfloat16).reshape(-1, model_width)
    )
    hidden = jax.nn.relu(jnp.dot(normed_two, up_weight, preferred_element_type=jnp.float32)).astype(
        jnp.bfloat16
    )
    output = jnp.dot(hidden, down_weight, preferred_element_type=jnp.float32)
    return state_after + output.reshape(state_after.shape)


def run_layer(seq_data, layer_index, w_attn, w_up, w_down, norm_gain, norm_bias, block_rows):
    seq_count, seq_length, inner_count, model_width = seq_data.shape
    per_block = math.gcd(seq_count, max(1, block_rows // (seq_length * inner_count)))
    pos_table = positions_table(seq_length, model_width)
    blocked = seq_data.reshape(
        seq_count // per_block, per_block, seq_length, inner_count, model_width
    )

    def apply_block(seq_block):
        return encoder_block(
            seq_block,
            pos_table,
            w_attn[layer_index],
            w_up[layer_index],
            w_down[layer_index],
            norm_gain[layer_index],
            norm_bias[layer_index],
        )

    return lax.map(apply_block, blocked).reshape(seq_count, seq_length, inner_count, model_width)


def group_norm(values, gain_row, bias_row):
    cell_count = (
        values.shape[1] * lax.axis_size(("wide", "narrow")) * values.shape[2] * values.shape[3]
    )
    totals, squares = lax.psum(
        (jnp.sum(values, axis=(1, 2, 3)), jnp.sum(values * values, axis=(1, 2, 3))),
        ("wide", "narrow"),
    )
    mean_flat = totals / cell_count
    variance = squares / cell_count - mean_flat * mean_flat
    centered = values - mean_flat[:, None, None, None]
    return centered * lax.rsqrt(variance[:, None, None, None] + EPSILON) * gain_row + bias_row


def on_device(mixture, w_attn, w_up, w_down, norm_gain, norm_bias, group_gain, group_bias):
    mix_count, segs_here, frame_count, model_width = mixture.shape
    intra_out = run_layer(
        mixture.reshape(mix_count * segs_here, frame_count, 1, model_width),
        0,
        w_attn,
        w_up,
        w_down,
        norm_gain,
        norm_bias,
        512,
    ).reshape(mixture.shape)
    carried = (
        group_norm(intra_out, group_gain[0], group_bias[0]) + mixture.astype(jnp.float32)
    ).astype(jnp.bfloat16)
    result = run_layer(
        lax.all_to_all(carried, ("wide", "narrow"), split_axis=2, concat_axis=1, tiled=True),
        1,
        w_attn,
        w_up,
        w_down,
        norm_gain,
        norm_bias,
        512,
    ).astype(jnp.bfloat16)
    inter_out = lax.all_to_all(result, ("wide", "narrow"), split_axis=1, concat_axis=2, tiled=True)
    separated = group_norm(
        inter_out.astype(jnp.float32), group_gain[1], group_bias[1]
    ) + carried.astype(jnp.float32)
    return separated.astype(jnp.bfloat16)


def fixed_positions(seq_length, model_width):
    positions = np.arange(seq_length, dtype=np.float64)[:, None]
    freq_index = np.arange(model_width // 2, dtype=np.float64)[None, :]
    angles = positions * np.exp(freq_index * (-2.0 * math.log(10000.0) / model_width))
    return np.concatenate([np.sin(angles), np.cos(angles)], axis=1).astype(np.float32)


def pick_sizes(mixture, device_count):
    _, segs_here, frame_count, model_width = mixture.shape
    seq_length = segs_here * device_count
    frames_here = frame_count // device_count
    group_rows = min(frame_count, seq_length * frames_here)
    fits = (
        frames_here == 8
        and frame_count % 128 == 0
        and 128 % seq_length == 0
        and group_rows % 128 == 0
        and (seq_length * frames_here) % group_rows == 0
        and model_width % 128 == 0
        and 128 % (model_width // HEADS) == 0
    )
    return fits, seq_length, frames_here, group_rows


def dot(left, right, left_dim=1, right_dim=0):
    return lax.dot_general(
        left, right, (((left_dim,), (right_dim,)), ((), ())), preferred_element_type=jnp.float32
    )


def group_layer(state_rows, seq_length, attn, up_weight, down_weight, gains, biases):
    rows, model_width = state_rows.shape
    head_size = model_width // HEADS
    heads_in_tile = 128 // head_size
    scale = math.log2(math.e) / math.sqrt(head_size)
    normed = layer_norm(state_rows, gains[0:1], biases[0:1]).astype(jnp.bfloat16)
    queries = (dot(attn(0), normed, 1, 1) * scale).astype(jnp.bfloat16)
    key_rows = dot(normed, attn(1)).astype(jnp.bfloat16)
    value_cols = dot(attn(2), normed, 1, 1).astype(jnp.bfloat16)
    zero_rows = jnp.zeros((head_size, rows), jnp.bfloat16)
    one_rows = jnp.ones((16, rows), jnp.bfloat16)
    packed = seq_length < rows
    if packed:
        lane_seq = lax.broadcasted_iota(jnp.int32, (seq_length, 128), 1) // seq_length
        seqs_in_tile = 128 // seq_length
    parts = []

    def score(head):
        tile, place = divmod(head, heads_in_tile)
        own = queries[head * head_size : (head + 1) * head_size]
        spread = jnp.concatenate(
            [own if i == place else zero_rows for i in range(heads_in_tile)], axis=0
        )
        return dot(key_rows[:, tile * 128 : (tile + 1) * 128], spread)

    def attend(head):
        own_values = value_cols[head * head_size : (head + 1) * head_size]
        attended = dot(jnp.concatenate([own_values, one_rows], axis=0), waiting[head])
        inverse = 1.0 / attended[head_size : head_size + 1]
        return (attended[:head_size] * inverse).astype(jnp.bfloat16)

    waiting = []
    ahead = [score(0), score(1)]
    for head in range(HEADS):
        scores = ahead[head]
        if head + 2 < HEADS:
            ahead.append(score(head + 2))
        if packed:
            columns = []
            for lane_tile in range(rows // 128):
                block = None
                for i in range(seqs_in_tile):
                    first = (lane_tile * seqs_in_tile + i) * seq_length
                    piece = scores[
                        first : first + seq_length, lane_tile * 128 : (lane_tile + 1) * 128
                    ]
                    block = piece if block is None else jnp.where(lane_seq == i, piece, block)
                columns.append(block)
            scores = jnp.concatenate(columns, axis=1)
        shifted = jnp.exp2(scores - jnp.max(scores, axis=0, keepdims=True))
        if packed:
            row_blocks = []
            for seq in range(rows // seq_length):
                lane_tile, i = divmod(seq, seqs_in_tile)
                kept = jnp.where(
                    lane_seq == i, shifted[:, lane_tile * 128 : (lane_tile + 1) * 128], 0.0
                )
                none = jnp.zeros_like(kept)
                row_blocks.append(
                    jnp.concatenate(
                        [kept if t == lane_tile else none for t in range(rows // 128)], axis=1
                    )
                )
            shifted = jnp.concatenate(row_blocks, axis=0)
        waiting.append(shifted.astype(jnp.bfloat16))
        if head >= 1:
            parts.append(attend(head - 1))
    parts.append(attend(HEADS - 1))
    mixed = dot(jnp.concatenate(parts, axis=0), attn(3), 0, 0)
    state_after = state_rows + mixed
    normed_two = layer_norm(state_after, gains[1:2], biases[1:2]).astype(jnp.bfloat16)
    hidden = jnp.maximum(dot(normed_two, up_weight), 0.0).astype(jnp.bfloat16)
    return state_after + dot(hidden, down_weight)


def lane_sums(values):
    column = jnp.sum(values, axis=0, keepdims=True)
    total = column[:, 0:128]
    for tile in range(1, values.shape[1] // 128):
        total = total + column[:, tile * 128 : (tile + 1) * 128]
    return total


def fused_kernel(
    axis_names,
    axis_sizes,
    seq_length,
    frames_here,
    group_rows,
    x_ref,
    attn_ref,
    up_ref,
    down_ref,
    ngain_ref,
    nbias_ref,
    ggain_ref,
    gbias_ref,
    pos0_ref,
    pos1_ref,
    out_ref,
    y_scr,
    carried_scr,
    recv_scr,
    inter_scr,
    back_scr,
    rows_scr,
    stat_scr,
    turned_scr,
    send_sem,
    recv_sem,
):
    mixes, segs_here, frame_count, model_width = x_ref.shape
    n = axis_sizes[0] * axis_sizes[1]
    me = lax.axis_index(axis_names[0]) * axis_sizes[1] + lax.axis_index(axis_names[1])
    cells = float(n * segs_here * frame_count * model_width)
    lane_tiles = model_width // 128

    def device_of(index):
        return (index // axis_sizes[1], lax.rem(index, axis_sizes[1]))

    barrier = pltpu.get_barrier_semaphore()

    def greet(k, carry):
        pl.semaphore_signal(
            barrier, inc=1, device_id=device_of(lax.rem(me + k, n)), device_id_type=MESH
        )
        return carry

    lax.fori_loop(1, n, greet, 0)

    for layer in range(2):
        for i in range(2):
            turned_scr[layer, i] = attn_ref[layer, 2 * i].T

    def send_all(kind, b, source, target):
        def send(k, carry):
            peer = lax.rem(me + k, n)
            pltpu.make_async_remote_copy(
                src_ref=source(peer),
                dst_ref=target(),
                send_sem=send_sem.at[kind, b],
                recv_sem=recv_sem.at[kind, b],
                device_id=device_of(peer),
                device_id_type=MESH,
            ).start()
            return carry

        lax.fori_loop(1, n, send, 0)

    def arrived(ref, sem):
        pltpu.make_async_copy(ref, ref, sem).wait()

    def stat_block(which, b):
        return stat_scr.at[which, b, pl.ds(0, n - 1)]

    def share_stats(which, b, sums, squares):
        stat_scr[which, b, me, 0:1, :] = sums
        stat_scr[which, b, me, 1:2, :] = squares
        send_all(
            which,
            b,
            lambda peer: stat_scr.at[which, b, me],
            lambda: stat_scr.at[which, b, me],
        )

    def affine(which, b):
        arrived(stat_block(which, b), recv_sem.at[which, b])
        total = jnp.sum(stat_scr[which, b], axis=0)
        flat = jnp.sum(total, axis=1, keepdims=True) / cells
        mean = flat[0:1]
        variance = flat[1:2] - mean * mean
        gain = lax.rsqrt(variance + EPSILON) * ggain_ref[which : which + 1]
        return gain, gbias_ref[which : which + 1] - mean * gain

    def weights(layer):
        return (
            lambda i: turned_scr[layer, i // 2] if i % 2 == 0 else attn_ref[layer, i],
            up_ref[layer],
            down_ref[layer],
            ngain_ref[layer],
            nbias_ref[layer],
        )

    def intra(b):
        def one(c, sums):
            state = x_ref[b, c].astype(jnp.float32) + pos0_ref[...]
            y = group_layer(state, frame_count, *weights(0))
            y_scr[b, c] = y
            return sums[0] + lane_sums(y), sums[1] + lane_sums(y * y)

        zero = jnp.zeros((1, 128), jnp.float32)
        return lax.fori_loop(0, segs_here, one, (zero, zero), unroll=True)

    def carry_out(b):
        gain, bias = affine(0, b)

        def one(c, carry):
            full = y_scr[b, c] * gain + bias + x_ref[b, c].astype(jnp.float32)
            carried_scr[b, c] = full.reshape(n, frames_here, model_width).astype(jnp.bfloat16)
            return carry

        lax.fori_loop(0, segs_here, one, 0)
        recv_scr[b, pl.ds(me * segs_here, segs_here)] = carried_scr[b, :, me]
        send_all(
            2,
            b,
            lambda peer: carried_scr.at[b, :, peer],
            lambda: recv_scr.at[b, pl.ds(me * segs_here, segs_here)],
        )

    def first_half(step, carry):
        @pl.when(step < mixes)
        def _():
            sums, squares = intra(step)

            @pl.when(step == 0)
            def _():
                pl.semaphore_wait(barrier, n - 1)

            share_stats(0, step, sums, squares)

        @pl.when(step >= 1)
        def _():
            carry_out(step - 1)

        return carry

    lax.fori_loop(0, mixes + 1, first_half, 0)

    seqs = group_rows // seq_length

    def inter(b, carry):
        arrived(recv_scr.at[b, pl.ds(0, (n - 1) * segs_here)], recv_sem.at[2, b])
        wide_rows = recv_scr[b].astype(jnp.float32).reshape(seq_length * frames_here, model_width)
        for t in range(lane_tiles):
            rows_scr[t] = wide_rows[:, t * 128 : (t + 1) * 128]

        def one(g, sums):
            blocks = []
            for i in range(seqs):
                picked = [
                    rows_scr[t, pl.ds(g * seqs + i, seq_length, stride=frames_here), :]
                    for t in range(lane_tiles)
                ]
                blocks.append(jnp.concatenate(picked, axis=1) + pos1_ref[...])
            y = group_layer(jnp.concatenate(blocks, axis=0), seq_length, *weights(1))
            y = y.astype(jnp.bfloat16).astype(jnp.float32)
            for i in range(seqs):
                for t in range(lane_tiles):
                    rows_scr[t, pl.ds(g * seqs + i, seq_length, stride=frames_here), :] = y[
                        i * seq_length : (i + 1) * seq_length, t * 128 : (t + 1) * 128
                    ]
            return sums[0] + lane_sums(y), sums[1] + lane_sums(y * y)

        zero = jnp.zeros((1, 128), jnp.float32)
        sums, squares = lax.fori_loop(0, frames_here // seqs, one, (zero, zero), unroll=True)
        for t in range(lane_tiles):
            inter_scr[b, :, :, t * 128 : (t + 1) * 128] = (
                rows_scr[t].reshape(seq_length, frames_here, 128).astype(jnp.bfloat16)
            )
        back_scr[b, :, me] = inter_scr[b, pl.ds(me * segs_here, segs_here)]
        share_stats(1, b, sums, squares)
        send_all(
            3,
            b,
            lambda peer: inter_scr.at[b, pl.ds(peer * segs_here, segs_here)],
            lambda: back_scr.at[b, :, me],
        )
        return carry

    lax.fori_loop(0, mixes, inter, 0)

    def finish(b, carry):
        gain, bias = affine(1, b)
        arrived(back_scr.at[b, :, pl.ds(0, n - 1)], recv_sem.at[3, b])

        def one(c, inner):
            full = back_scr[b, c].astype(jnp.float32) * gain + bias
            full = full + carried_scr[b, c].astype(jnp.float32)
            out_ref[b, c] = full.reshape(frame_count, model_width).astype(jnp.bfloat16)
            return inner

        lax.fori_loop(0, segs_here, one, 0)
        arrived(stat_block(0, b), send_sem.at[0, b])
        arrived(stat_block(1, b), send_sem.at[1, b])
        arrived(carried_scr.at[b, :, pl.ds(0, n - 1)], send_sem.at[2, b])
        arrived(inter_scr.at[b, pl.ds(0, (n - 1) * segs_here)], send_sem.at[3, b])
        return carry

    lax.fori_loop(0, mixes, finish, 0)


def fused(mesh, mixture, w_attn, w_up, w_down, norm_gain, norm_bias, group_gain, group_bias):
    axis_names = ("wide", "narrow")
    axis_sizes = tuple(mesh.shape[name] for name in axis_names)
    n = axis_sizes[0] * axis_sizes[1]
    mixes, segs_here, frame_count, model_width = mixture.shape
    _, seq_length, frames_here, group_rows = pick_sizes(mixture, n)
    split = (mixes, segs_here, n, frames_here, model_width)
    joined = (mixes, seq_length, frames_here, model_width)
    return pl.pallas_call(
        functools.partial(
            fused_kernel, axis_names, axis_sizes, seq_length, frames_here, group_rows
        ),
        out_shape=jax.ShapeDtypeStruct(mixture.shape, jnp.bfloat16),
        in_specs=[pl.BlockSpec(memory_space=pltpu.VMEM)] * 10,
        out_specs=pl.BlockSpec(memory_space=pltpu.VMEM),
        scratch_shapes=[
            pltpu.VMEM(mixture.shape, jnp.float32),
            pltpu.VMEM(split, jnp.bfloat16),
            pltpu.VMEM(joined, jnp.bfloat16),
            pltpu.VMEM(joined, jnp.bfloat16),
            pltpu.VMEM(split, jnp.bfloat16),
            pltpu.VMEM((model_width // 128, seq_length * frames_here, 128), jnp.float32),
            pltpu.VMEM((2, mixes, n, 2, 128), jnp.float32),
            pltpu.VMEM((2, 2, model_width, model_width), jnp.bfloat16),
            pltpu.SemaphoreType.DMA((4, mixes)),
            pltpu.SemaphoreType.DMA((4, mixes)),
        ],
        compiler_params=pltpu.CompilerParams(
            collective_id=0, has_side_effects=True, vmem_limit_bytes=60 * 1024 * 1024
        ),
    )(
        mixture,
        w_attn,
        w_up,
        w_down,
        norm_gain,
        norm_bias,
        group_gain,
        group_bias,
        jnp.asarray(fixed_positions(frame_count, model_width)),
        jnp.asarray(fixed_positions(seq_length, model_width)),
    )


def solution(mesh):
    in_specs = (P(None, ("wide", "narrow"), None, None), P(), P(), P(), P(), P(), P(), P())
    out_specs = P(None, ("wide", "narrow"), None, None)

    def step(mixture, *parameters):
        device_count = mesh.shape["wide"] * mesh.shape["narrow"]
        if pick_sizes(mixture, device_count)[0]:
            return fused(mesh, mixture, *parameters)
        return on_device(mixture, *parameters)

    return jax.shard_map(step, mesh=mesh, in_specs=in_specs, out_specs=out_specs, check_vma=False)
```

```python
import functools
import math

import jax
import jax.numpy as jnp
import numpy as np
from jax import lax
from jax.experimental import pallas as pl
from jax.experimental.pallas import tpu as pltpu
from jax.sharding import PartitionSpec as P

HEADS = 8
MESH = pl.DeviceIdType.MESH


EPSILON = 1e-05


def positions_table(seq_length, model_width):
    positions = jnp.arange(seq_length, dtype=jnp.float32)[:, None]
    freq_index = jnp.arange(model_width // 2, dtype=jnp.float32)[None, :]
    angles = positions * jnp.exp(freq_index * (-2.0 * math.log(10000.0) / model_width))
    return jnp.concatenate([jnp.sin(angles), jnp.cos(angles)], axis=1)


def layer_norm(values, gain_row, bias_row):
    mean_value = jnp.mean(values, axis=-1, keepdims=True)
    centered = values - mean_value
    variance = jnp.mean(centered * centered, axis=-1, keepdims=True)
    return centered * lax.rsqrt(variance + EPSILON) * gain_row + bias_row


def encoder_block(seq_block, pos_table, attn_weights, up_weight, down_weight, gains, biases):
    groups, seq_length, inner_count, model_width = seq_block.shape
    head_size = model_width // HEADS
    state_rows = seq_block.astype(jnp.float32) + pos_table[None, :, None, :]
    normed = (
        layer_norm(state_rows, gains[0], biases[0]).astype(jnp.bfloat16).reshape(-1, model_width)
    )

    def project(matrix):
        product = jnp.dot(normed, matrix, preferred_element_type=jnp.float32).astype(jnp.bfloat16)
        return product.reshape(groups, seq_length, inner_count, HEADS, head_size)

    queries = project(attn_weights[0])
    key_rows = project(attn_weights[1])
    value_rows = project(attn_weights[2])
    scores = jnp.einsum("alnhe,amnhe->anhlm", queries, key_rows, preferred_element_type=jnp.float32)
    scores = scores * (1.0 / math.sqrt(head_size))
    shifted = jnp.exp(scores - jnp.max(scores, axis=-1, keepdims=True))
    weights = (shifted / jnp.sum(shifted, axis=-1, keepdims=True)).astype(jnp.bfloat16)
    attended = jnp.einsum(
        "anhlm,amnhe->alnhe", weights, value_rows, preferred_element_type=jnp.float32
    )
    attended = attended.astype(jnp.bfloat16).reshape(-1, model_width)
    mixed = jnp.dot(attended, attn_weights[3], preferred_element_type=jnp.float32)
    state_after = state_rows + mixed.reshape(state_rows.shape)
    normed_two = (
        layer_norm(state_after, gains[1], biases[1]).astype(jnp.bfloat16).reshape(-1, model_width)
    )
    hidden = jax.nn.relu(jnp.dot(normed_two, up_weight, preferred_element_type=jnp.float32)).astype(
        jnp.bfloat16
    )
    output = jnp.dot(hidden, down_weight, preferred_element_type=jnp.float32)
    return state_after + output.reshape(state_after.shape)


def run_layer(seq_data, layer_index, w_attn, w_up, w_down, norm_gain, norm_bias, block_rows):
    seq_count, seq_length, inner_count, model_width = seq_data.shape
    per_block = math.gcd(seq_count, max(1, block_rows // (seq_length * inner_count)))
    pos_table = positions_table(seq_length, model_width)
    blocked = seq_data.reshape(
        seq_count // per_block, per_block, seq_length, inner_count, model_width
    )

    def apply_block(seq_block):
        return encoder_block(
            seq_block,
            pos_table,
            w_attn[layer_index],
            w_up[layer_index],
            w_down[layer_index],
            norm_gain[layer_index],
            norm_bias[layer_index],
        )

    return lax.map(apply_block, blocked).reshape(seq_count, seq_length, inner_count, model_width)


def group_norm(values, gain_row, bias_row):
    cell_count = (
        values.shape[1] * lax.axis_size(("wide", "narrow")) * values.shape[2] * values.shape[3]
    )
    totals, squares = lax.psum(
        (jnp.sum(values, axis=(1, 2, 3)), jnp.sum(values * values, axis=(1, 2, 3))),
        ("wide", "narrow"),
    )
    mean_flat = totals / cell_count
    variance = squares / cell_count - mean_flat * mean_flat
    centered = values - mean_flat[:, None, None, None]
    return centered * lax.rsqrt(variance[:, None, None, None] + EPSILON) * gain_row + bias_row


def on_device(mixture, w_attn, w_up, w_down, norm_gain, norm_bias, group_gain, group_bias):
    mix_count, segs_here, frame_count, model_width = mixture.shape
    intra_out = run_layer(
        mixture.reshape(mix_count * segs_here, frame_count, 1, model_width),
        0,
        w_attn,
        w_up,
        w_down,
        norm_gain,
        norm_bias,
        512,
    ).reshape(mixture.shape)
    carried = (
        group_norm(intra_out, group_gain[0], group_bias[0]) + mixture.astype(jnp.float32)
    ).astype(jnp.bfloat16)
    result = run_layer(
        lax.all_to_all(carried, ("wide", "narrow"), split_axis=2, concat_axis=1, tiled=True),
        1,
        w_attn,
        w_up,
        w_down,
        norm_gain,
        norm_bias,
        512,
    ).astype(jnp.bfloat16)
    inter_out = lax.all_to_all(result, ("wide", "narrow"), split_axis=1, concat_axis=2, tiled=True)
    separated = group_norm(
        inter_out.astype(jnp.float32), group_gain[1], group_bias[1]
    ) + carried.astype(jnp.float32)
    return separated.astype(jnp.bfloat16)


def fixed_positions(seq_length, model_width):
    positions = np.arange(seq_length, dtype=np.float64)[:, None]
    freq_index = np.arange(model_width // 2, dtype=np.float64)[None, :]
    angles = positions * np.exp(freq_index * (-2.0 * math.log(10000.0) / model_width))
    return np.concatenate([np.sin(angles), np.cos(angles)], axis=1).astype(np.float32)


def pick_sizes(mixture, device_count):
    _, segs_here, frame_count, model_width = mixture.shape
    seq_length = segs_here * device_count
    frames_here = frame_count // device_count
    group_rows = min(frame_count, seq_length * frames_here)
    fits = (
        frames_here == 8
        and frame_count % 128 == 0
        and 128 % seq_length == 0
        and group_rows % 128 == 0
        and (seq_length * frames_here) % group_rows == 0
        and model_width % 128 == 0
        and 128 % (model_width // HEADS) == 0
    )
    return fits, seq_length, frames_here, group_rows


def dot(left, right, left_dim=1, right_dim=0):
    return lax.dot_general(
        left, right, (((left_dim,), (right_dim,)), ((), ())), preferred_element_type=jnp.float32
    )


def group_layer(state_rows, seq_length, attn, up_weight, down_weight, gains, biases):
    rows, model_width = state_rows.shape
    head_size = model_width // HEADS
    heads_in_tile = 128 // head_size
    scale = math.log2(math.e) / math.sqrt(head_size)
    normed = layer_norm(state_rows, gains[0:1], biases[0:1]).astype(jnp.bfloat16)
    queries = (dot(attn(0), normed, 1, 1) * scale).astype(jnp.bfloat16)
    key_rows = dot(normed, attn(1)).astype(jnp.bfloat16)
    value_cols = dot(attn(2), normed, 1, 1).astype(jnp.bfloat16)
    zero_rows = jnp.zeros((head_size, rows), jnp.bfloat16)
    one_rows = jnp.ones((16, rows), jnp.bfloat16)
    packed = seq_length < rows
    if packed:
        lane_seq = lax.broadcasted_iota(jnp.int32, (seq_length, 128), 1) // seq_length
        seqs_in_tile = 128 // seq_length
    parts = []

    def score(head):
        tile, place = divmod(head, heads_in_tile)
        own = queries[head * head_size : (head + 1) * head_size]
        spread = jnp.concatenate(
            [own if i == place else zero_rows for i in range(heads_in_tile)], axis=0
        )
        return dot(key_rows[:, tile * 128 : (tile + 1) * 128], spread)

    def attend(head):
        own_values = value_cols[head * head_size : (head + 1) * head_size]
        attended = dot(jnp.concatenate([own_values, one_rows], axis=0), waiting[head])
        inverse = 1.0 / attended[head_size : head_size + 1]
        return (attended[:head_size] * inverse).astype(jnp.bfloat16)

    waiting = []
    ahead = [score(0), score(1)]
    for head in range(HEADS):
        scores = ahead[head]
        if head + 2 < HEADS:
            ahead.append(score(head + 2))
        if packed:
            columns = []
            for lane_tile in range(rows // 128):
                block = None
                for i in range(seqs_in_tile):
                    first = (lane_tile * seqs_in_tile + i) * seq_length
                    piece = scores[
                        first : first + seq_length, lane_tile * 128 : (lane_tile + 1) * 128
                    ]
                    block = piece if block is None else jnp.where(lane_seq == i, piece, block)
                columns.append(block)
            scores = jnp.concatenate(columns, axis=1)
        shifted = jnp.exp2(scores - jnp.max(scores, axis=0, keepdims=True))
        if packed:
            row_blocks = []
            for seq in range(rows // seq_length):
                lane_tile, i = divmod(seq, seqs_in_tile)
                kept = jnp.where(
                    lane_seq == i, shifted[:, lane_tile * 128 : (lane_tile + 1) * 128], 0.0
                )
                none = jnp.zeros_like(kept)
                row_blocks.append(
                    jnp.concatenate(
                        [kept if t == lane_tile else none for t in range(rows // 128)], axis=1
                    )
                )
            shifted = jnp.concatenate(row_blocks, axis=0)
        waiting.append(shifted.astype(jnp.bfloat16))
        if head >= 1:
            parts.append(attend(head - 1))
    parts.append(attend(HEADS - 1))
    mixed = dot(jnp.concatenate(parts, axis=0), attn(3), 0, 0)
    state_after = state_rows + mixed
    normed_two = layer_norm(state_after, gains[1:2], biases[1:2]).astype(jnp.bfloat16)
    hidden = jnp.maximum(dot(normed_two, up_weight), 0.0).astype(jnp.bfloat16)
    return state_after + dot(hidden, down_weight)


def lane_sums(values):
    column = jnp.sum(values, axis=0, keepdims=True)
    total = column[:, 0:128]
    for tile in range(1, values.shape[1] // 128):
        total = total + column[:, tile * 128 : (tile + 1) * 128]
    return total


def fused_kernel(
    axis_names,
    axis_sizes,
    seq_length,
    frames_here,
    group_rows,
    x_ref,
    attn_ref,
    up_ref,
    down_ref,
    ngain_ref,
    nbias_ref,
    ggain_ref,
    gbias_ref,
    pos0_ref,
    pos1_ref,
    out_ref,
    y_scr,
    carried_scr,
    recv_scr,
    inter_scr,
    back_scr,
    rows_scr,
    stat_scr,
    turned_scr,
    send_sem,
    recv_sem,
):
    mixes, segs_here, frame_count, model_width = x_ref.shape
    n = axis_sizes[0] * axis_sizes[1]
    me = lax.axis_index(axis_names[0]) * axis_sizes[1] + lax.axis_index(axis_names[1])
    cells = float(n * segs_here * frame_count * model_width)
    lane_tiles = model_width // 128

    def device_of(index):
        return (index // axis_sizes[1], lax.rem(index, axis_sizes[1]))

    barrier = pltpu.get_barrier_semaphore()

    def greet(k, carry):
        pl.semaphore_signal(
            barrier, inc=1, device_id=device_of(lax.rem(me + k, n)), device_id_type=MESH
        )
        return carry

    lax.fori_loop(1, n, greet, 0, unroll=True)

    for layer in range(2):
        for i in range(2):
            turned_scr[layer, i] = attn_ref[layer, 2 * i].T

    def send_all(kind, b, source, target):
        def send(k, carry):
            peer = lax.rem(me + k, n)
            pltpu.make_async_remote_copy(
                src_ref=source(peer),
                dst_ref=target(),
                send_sem=send_sem.at[kind, b],
                recv_sem=recv_sem.at[kind, b],
                device_id=device_of(peer),
                device_id_type=MESH,
            ).start()
            return carry

        lax.fori_loop(1, n, send, 0, unroll=True)

    def arrived(ref, sem):
        pltpu.make_async_copy(ref, ref, sem).wait()

    def stat_block(which, b):
        return stat_scr.at[which, b, pl.ds(0, n - 1)]

    def share_stats(which, b, sums, squares):
        stat_scr[which, b, me, 0:1, :] = sums
        stat_scr[which, b, me, 1:2, :] = squares
        send_all(
            which,
            b,
            lambda peer: stat_scr.at[which, b, me],
            lambda: stat_scr.at[which, b, me],
        )

    def affine(which, b):
        arrived(stat_block(which, b), recv_sem.at[which, b])
        total = jnp.sum(stat_scr[which, b], axis=0)
        flat = jnp.sum(total, axis=1, keepdims=True) / cells
        mean = flat[0:1]
        variance = flat[1:2] - mean * mean
        gain = lax.rsqrt(variance + EPSILON) * ggain_ref[which : which + 1]
        return gain, gbias_ref[which : which + 1] - mean * gain

    def weights(layer):
        return (
            lambda i: turned_scr[layer, i // 2] if i % 2 == 0 else attn_ref[layer, i],
            up_ref[layer],
            down_ref[layer],
            ngain_ref[layer],
            nbias_ref[layer],
        )

    def intra(b):
        def one(c, sums):
            state = x_ref[b, c].astype(jnp.float32) + pos0_ref[...]
            y = group_layer(state, frame_count, *weights(0))
            y_scr[b, c] = y
            return sums[0] + lane_sums(y), sums[1] + lane_sums(y * y)

        zero = jnp.zeros((1, 128), jnp.float32)
        return lax.fori_loop(0, segs_here, one, (zero, zero), unroll=True)

    def carry_out(b):
        gain, bias = affine(0, b)

        def one(c, carry):
            full = y_scr[b, c] * gain + bias + x_ref[b, c].astype(jnp.float32)
            carried_scr[b, c] = full.reshape(n, frames_here, model_width).astype(jnp.bfloat16)
            return carry

        lax.fori_loop(0, segs_here, one, 0)
        recv_scr[b, pl.ds(me * segs_here, segs_here)] = carried_scr[b, :, me]
        send_all(
            2,
            b,
            lambda peer: carried_scr.at[b, :, peer],
            lambda: recv_scr.at[b, pl.ds(me * segs_here, segs_here)],
        )

    def first_half(step, carry):
        @pl.when(step < mixes)
        def _():
            sums, squares = intra(step)

            @pl.when(step == 0)
            def _():
                pl.semaphore_wait(barrier, n - 1)

            share_stats(0, step, sums, squares)

        @pl.when(step >= 1)
        def _():
            carry_out(step - 1)

        return carry

    lax.fori_loop(0, mixes + 1, first_half, 0)

    seqs = group_rows // seq_length

    def inter(b, carry):
        arrived(recv_scr.at[b, pl.ds(0, (n - 1) * segs_here)], recv_sem.at[2, b])
        wide_rows = recv_scr[b].astype(jnp.float32).reshape(seq_length * frames_here, model_width)
        for t in range(lane_tiles):
            rows_scr[t] = wide_rows[:, t * 128 : (t + 1) * 128]

        def one(g, sums):
            blocks = []
            for i in range(seqs):
                picked = [
                    rows_scr[t, pl.ds(g * seqs + i, seq_length, stride=frames_here), :]
                    for t in range(lane_tiles)
                ]
                blocks.append(jnp.concatenate(picked, axis=1) + pos1_ref[...])
            y = group_layer(jnp.concatenate(blocks, axis=0), seq_length, *weights(1))
            y = y.astype(jnp.bfloat16).astype(jnp.float32)
            for i in range(seqs):
                for t in range(lane_tiles):
                    rows_scr[t, pl.ds(g * seqs + i, seq_length, stride=frames_here), :] = y[
                        i * seq_length : (i + 1) * seq_length, t * 128 : (t + 1) * 128
                    ]
            return sums[0] + lane_sums(y), sums[1] + lane_sums(y * y)

        zero = jnp.zeros((1, 128), jnp.float32)
        sums, squares = lax.fori_loop(0, frames_here // seqs, one, (zero, zero), unroll=True)
        for t in range(lane_tiles):
            inter_scr[b, :, :, t * 128 : (t + 1) * 128] = (
                rows_scr[t].reshape(seq_length, frames_here, 128).astype(jnp.bfloat16)
            )
        back_scr[b, :, me] = inter_scr[b, pl.ds(me * segs_here, segs_here)]
        share_stats(1, b, sums, squares)
        send_all(
            3,
            b,
            lambda peer: inter_scr.at[b, pl.ds(peer * segs_here, segs_here)],
            lambda: back_scr.at[b, :, me],
        )
        return carry

    lax.fori_loop(0, mixes, inter, 0)

    def finish(b, carry):
        gain, bias = affine(1, b)
        arrived(back_scr.at[b, :, pl.ds(0, n - 1)], recv_sem.at[3, b])

        def one(c, inner):
            full = back_scr[b, c].astype(jnp.float32) * gain + bias
            full = full + carried_scr[b, c].astype(jnp.float32)
            out_ref[b, c] = full.reshape(frame_count, model_width).astype(jnp.bfloat16)
            return inner

        lax.fori_loop(0, segs_here, one, 0)
        arrived(stat_block(0, b), send_sem.at[0, b])
        arrived(stat_block(1, b), send_sem.at[1, b])
        arrived(carried_scr.at[b, :, pl.ds(0, n - 1)], send_sem.at[2, b])
        arrived(inter_scr.at[b, pl.ds(0, (n - 1) * segs_here)], send_sem.at[3, b])
        return carry

    lax.fori_loop(0, mixes, finish, 0)


def fused(mesh, mixture, w_attn, w_up, w_down, norm_gain, norm_bias, group_gain, group_bias):
    axis_names = ("wide", "narrow")
    axis_sizes = tuple(mesh.shape[name] for name in axis_names)
    n = axis_sizes[0] * axis_sizes[1]
    mixes, segs_here, frame_count, model_width = mixture.shape
    _, seq_length, frames_here, group_rows = pick_sizes(mixture, n)
    split = (mixes, segs_here, n, frames_here, model_width)
    joined = (mixes, seq_length, frames_here, model_width)
    return pl.pallas_call(
        functools.partial(
            fused_kernel, axis_names, axis_sizes, seq_length, frames_here, group_rows
        ),
        out_shape=jax.ShapeDtypeStruct(mixture.shape, jnp.bfloat16),
        in_specs=[pl.BlockSpec(memory_space=pltpu.VMEM)] * 10,
        out_specs=pl.BlockSpec(memory_space=pltpu.VMEM),
        scratch_shapes=[
            pltpu.VMEM(mixture.shape, jnp.float32),
            pltpu.VMEM(split, jnp.bfloat16),
            pltpu.VMEM(joined, jnp.bfloat16),
            pltpu.VMEM(joined, jnp.bfloat16),
            pltpu.VMEM(split, jnp.bfloat16),
            pltpu.VMEM((model_width // 128, seq_length * frames_here, 128), jnp.float32),
            pltpu.VMEM((2, mixes, n, 2, 128), jnp.float32),
            pltpu.VMEM((2, 2, model_width, model_width), jnp.bfloat16),
            pltpu.SemaphoreType.DMA((4, mixes)),
            pltpu.SemaphoreType.DMA((4, mixes)),
        ],
        compiler_params=pltpu.CompilerParams(
            collective_id=0, has_side_effects=True, vmem_limit_bytes=60 * 1024 * 1024
        ),
    )(
        mixture,
        w_attn,
        w_up,
        w_down,
        norm_gain,
        norm_bias,
        group_gain,
        group_bias,
        jnp.asarray(fixed_positions(frame_count, model_width)),
        jnp.asarray(fixed_positions(seq_length, model_width)),
    )


def solution(mesh):
    in_specs = (P(None, ("wide", "narrow"), None, None), P(), P(), P(), P(), P(), P(), P())
    out_specs = P(None, ("wide", "narrow"), None, None)

    def step(mixture, *parameters):
        device_count = mesh.shape["wide"] * mesh.shape["narrow"]
        if pick_sizes(mixture, device_count)[0]:
            return fused(mesh, mixture, *parameters)
        return on_device(mixture, *parameters)

    return jax.shard_map(step, mesh=mesh, in_specs=in_specs, out_specs=out_specs, check_vma=False)
```
